32 devices in a mesh: dp: 32 (over z, y, x, core).
Axes of the slice: x: 2, y: 2, z: 4, core: 2. Of those that a mesh axis runs over, the one named last changes fastest.
Arguments:
- params: float32 [4063232], P('dp'), may hold values from -6 to 6
- first_moment: float32 [4063232], P('dp'), may hold values from -2 to 2
- second_moment: float32 [4063232], P('dp'), may hold values from 0.01 to 1
- grads: bfloat16 [4063232], P('dp'), may hold values from -6 to 6
- old_bounds: int32 [33], replicated, may hold values from 0 to 3932160, as said below
- new_bounds: int32 [33], replicated, may hold values from 0 to 3932160, as said below
- seg_start: int32 [64], replicated, may hold values from 0 to 3932096, as said below
Outputs:
- new_params: float32 [4063232], P('dp')
- new_first: float32 [4063232], P('dp')
- new_second: float32 [4063232], P('dp')
The draws below stay inside these ranges and needn't reach their ends.
Inputs may be any that keep to these rules, and one draw needn't show every extreme that they name: `old_bounds`: starts at 0 and ends at 3932160; every shard holds between 118784 and 126976 elements, exactly 126976 in some shard. `new_bounds`: starts at 0 and ends at 3932160; every shard holds between 118784 and 126976 elements, exactly 126976 in some shard; each entry differs from the same entry of old_bounds by at most 4096, by exactly 4096 somewhere. `seg_start`: strictly rising, the first is 0, all are multiples of 64.
All inputs are finite; a program needn't handle non-finite values.
Results may differ from the reference program's by a relative error of at most 0.0003.
Values sent between devices are 32-bit elements; how exact they have to be, the bound alone decides.
A program may use at most 64 MiB of HBM per device.

```python
import math
import jax
import jax.numpy as jnp

BASE = 122880
MARGIN = 4096
SEGS = 64
CAP = 126976
TOTAL = 3932160
N_DP = 32


def bounds_pair(key):
    half = MARGIN // 2
    first = jax.random.randint(jax.random.fold_in(key, 11), (N_DP + 1,), -half, half + 1)
    second = jax.random.randint(jax.random.fold_in(key, 12), (N_DP + 1,), -half, half + 1)
    where_at = jax.random.randint(jax.random.fold_in(key, 13), (), 1, N_DP - 2)
    index = jnp.arange(N_DP + 1, dtype=jnp.int32)
    first = jnp.where(index == where_at, -half, first)
    first = jnp.where(index == where_at + 1, half, first)
    second = jnp.where(index == where_at + 1, -half, second)
    second = jnp.where(index == where_at + 2, half, second)
    edges = (index == 0) | (index == N_DP)
    first = jnp.where(edges, 0, first)
    second = jnp.where(edges, 0, second)
    nominal = index * BASE
    return ((nominal + first).astype(jnp.int32), (nominal + second).astype(jnp.int32))


def draw_old_bounds(key, part):
    return bounds_pair(key)[0]


def draw_new_bounds(key, part):
    return bounds_pair(key)[1]


def draw_seg_start(key, part):
    picks = jax.random.permutation(jax.random.fold_in(key, 21), TOTAL // 64 - 1)[:SEGS - 1] + 1
    picks = jnp.sort(picks.astype(jnp.int32))
    return jnp.concatenate([jnp.zeros((1,), jnp.int32), picks * 64]).astype(jnp.int32)


def level_of(rng, dims, cuts, least, largest):
    loudness = 1.0
    for dim, blocks in cuts:
        heights = jax.random.uniform(jax.random.fold_in(jax.random.fold_in(rng, 6), dim), (blocks,), jnp.float32, least / len(cuts), largest / len(cuts))
        loudness = loudness * jnp.repeat(jnp.exp(heights), dims[dim] // blocks).reshape((-1,) + (1,) * (len(dims) - 1 - dim))
    return loudness


def normal_values(key, extent, spread, bound, pieces=(), kind=jnp.bfloat16):
    level = level_of(key, extent, pieces, -0.22, 0.18) if pieces else 1.0
    result = jax.random.normal(key, extent, jnp.float32) * spread * level
    return jnp.minimum(jnp.maximum(result, -bound), bound).astype(kind)


def setup_inputs(seed: int = 0) -> dict:
    streams_of = jax.random.split(jax.random.key(seed), 8)
    params = normal_values(streams_of[0], (N_DP * CAP,), 1.0, 6.0, ((0, 32),), jnp.float32)
    first_moment = normal_values(streams_of[1], (N_DP * CAP,), 0.3, 2.0, ((0, 32),), jnp.float32)
    second_moment = jnp.clip(jnp.exp(math.log(1.0) - 4.6051702 * jax.random.uniform(streams_of[2], (N_DP * CAP,), jnp.float32) ** level_of(streams_of[2], (N_DP * CAP,), ((0, 32),), -0.2, 0.2)), 0.01, 1.0)
    grads = normal_values(streams_of[3], (N_DP * CAP,), 1.0, 6.0, ((0, 32),))
    old_bounds = draw_old_bounds(jax.random.fold_in(streams_of[7], 71), 0)
    new_bounds = draw_new_bounds(jax.random.fold_in(streams_of[7], 71), 0)
    seg_start = draw_seg_start(jax.random.fold_in(streams_of[7], 71), 0)
    return {"params": params, "first_moment": first_moment, "second_moment": second_moment, "grads": grads, "old_bounds": old_bounds, "new_bounds": new_bounds, "seg_start": seg_start}


BETA_ONE = 0.9
BETA_TWO = 0.999
CORR_ONE = 1.0 - 0.9 ** 10
CORR_TWO = 1.0 - 0.999 ** 10
DECAY = 0.01
LEARN = 0.1
EPSILON = 1e-06

def reference(params, first_moment, second_moment, grads, old_bounds, new_bounds, seg_start):
    count = N_DP
    cap = BASE + MARGIN
    total = BASE * N_DP
    position = jnp.arange(total, dtype=jnp.int32)
    owner = (jnp.searchsorted(old_bounds, position, side='right') - 1).astype(jnp.int32)
    owner = jnp.clip(owner, 0, count - 1).astype(jnp.int32)
    source = (owner * cap + (position - old_bounds[owner])).astype(jnp.int32)
    weight = params[source]
    moment = first_moment[source]
    second = second_moment[source]
    gradient = grads[source].astype(jnp.float32)
    moment_new = BETA_ONE * moment + (1.0 - BETA_ONE) * gradient
    second_new = BETA_TWO * second + (1.0 - BETA_TWO) * gradient * gradient
    update = moment_new / CORR_ONE / (jnp.sqrt(second_new / CORR_TWO) + EPSILON) + DECAY * weight
    segment = (jnp.searchsorted(seg_start, position, side='right') - 1).astype(jnp.int32)
    weight_sq = jax.ops.segment_sum(weight * weight, segment, num_segments=SEGS)
    update_sq = jax.ops.segment_sum(update * update, segment, num_segments=SEGS)
    ratio = jnp.sqrt(weight_sq) / (jnp.sqrt(update_sq) + EPSILON)
    weight_new = weight - LEARN * ratio[segment] * update
    slot_index = jnp.arange(count * cap, dtype=jnp.int32)
    device = (slot_index // cap).astype(jnp.int32)
    within = (slot_index % cap).astype(jnp.int32)
    valid = within < new_bounds[device + 1] - new_bounds[device]
    target = jnp.clip(new_bounds[device] + within, 0, total - 1).astype(jnp.int32)
    zero = jnp.float32(0.0)
    return (jnp.where(valid, weight_new[target], zero), jnp.where(valid, moment_new[target], zero), jnp.where(valid, second_new[target], zero))
```

```python
import functools

import jax
import jax.numpy as jnp
from jax import lax
from jax.experimental import pallas as pl
from jax.experimental.pallas import tpu as pltpu
from jax.sharding import PartitionSpec as P

MARGIN = 4096
LANES = 128
BLOCK = MARGIN // LANES
PAD = BLOCK + 8
EDGE = 2 * PAD + BLOCK


BETA_ONE = 0.9
BETA_TWO = 0.999
CORR_ONE = 1.0 - 0.9**10
CORR_TWO = 1.0 - 0.999**10
DECAY = 0.01
LEARN = 0.1
EPSILON = 1e-06

MESH = pl.DeviceIdType.MESH
VMEM_LIMIT = 16 * 1024 * 1024


def lane_ids(rows=BLOCK):
    return lax.broadcasted_iota(jnp.int32, (rows, LANES), 1)


def flat_ids():
    return lax.broadcasted_iota(jnp.int32, (BLOCK, LANES), 0) * LANES + lane_ids()


def moved(first, second, lanes):
    picked = jnp.where(lane_ids() >= lanes, first, second)
    return pltpu.roll(picked, (LANES - lanes) & (LANES - 1), 1)


def overlapping(seg_ref, low, high):
    def step(s, carry):
        first, end = carry
        start = seg_ref[s]
        return (first + (start <= low).astype(jnp.int32), end + (start < high).astype(jnp.int32))

    first, end = lax.fori_loop(0, seg_ref.shape[0], step, (jnp.int32(-1), jnp.int32(0)), unroll=8)
    return first, end


def span_of(seg_ref, s, low, count):
    segs = seg_ref.shape[0]
    begin = jnp.maximum(seg_ref[s] - low, 0)
    after = seg_ref[jnp.minimum(s + 1, segs - 1)] - low
    finish = jnp.where(s + 1 < segs, jnp.minimum(after, count), count)
    return begin, finish


def update_kernel(axis, old_ref, seg_ref, w_hbm, m_hbm, v_hbm, g_hbm, state, part, tail, head, m_buf, v_buf, g_buf, sems):
    rows = m_buf.shape[0]
    blocks = rows // BLOCK
    step_blocks = -(-blocks // sems.shape[1])
    chunks = [(b, min(b + step_blocks, blocks)) for b in range(0, blocks, step_blocks)]
    copies = []
    for c, (b0, b1) in enumerate(chunks):
        window = pl.ds(b0 * BLOCK, (b1 - b0) * BLOCK)
        placed = state.at[0, pl.ds(PAD + b0 * BLOCK, (b1 - b0) * BLOCK)]
        group = [
            pltpu.make_async_copy(w_hbm.at[window], placed, sems.at[0, c]),
            pltpu.make_async_copy(m_hbm.at[window], m_buf.at[window], sems.at[1, c]),
            pltpu.make_async_copy(v_hbm.at[window], v_buf.at[window], sems.at[2, c]),
            pltpu.make_async_copy(g_hbm.at[window], g_buf.at[window], sems.at[3, c]),
        ]
        for copy in group:
            copy.start()
        copies.append(group)

    me = lax.axis_index(axis)
    low = old_ref[me]
    high = old_ref[me + 1]
    count = high - low
    first, end = overlapping(seg_ref, low, high)

    def advance(b, carry):
        here = pl.multiple_of(b * BLOCK, BLOCK)
        there = pl.multiple_of(b * BLOCK + PAD, 8)
        gradient = g_buf[pl.ds(here, BLOCK), :].astype(jnp.float32)
        weight = state[0, pl.ds(there, BLOCK), :]
        moment = BETA_ONE * m_buf[pl.ds(here, BLOCK), :] + (1.0 - BETA_ONE) * gradient
        second = BETA_TWO * v_buf[pl.ds(here, BLOCK), :] + (1.0 - BETA_TWO) * gradient * gradient
        scaled = moment * (1.0 / CORR_ONE)
        update = scaled / (jnp.sqrt(second * (1.0 / CORR_TWO)) + EPSILON) + DECAY * weight
        state[1, pl.ds(there, BLOCK), :] = update
        state[2, pl.ds(there, BLOCK), :] = moment
        state[3, pl.ds(there, BLOCK), :] = second
        return carry

    for (b0, b1), group in zip(chunks, copies):
        for copy in group:
            copy.wait()
        lax.fori_loop(b0, b1, advance, 0)

    flat = flat_ids()
    lane = lane_ids(1)
    segs = seg_ref.shape[0]

    def tensor(s, row):
        begin, finish = span_of(seg_ref, s, low, count)

        def add(b, carry):
            there = pl.multiple_of(b * BLOCK + PAD, 8)
            index = flat + b * MARGIN
            inside = (index >= begin) & (index < finish)
            weight = state[0, pl.ds(there, BLOCK), :]
            update = state[1, pl.ds(there, BLOCK), :]
            return (
                carry[0] + jnp.where(inside, weight * weight, 0.0),
                carry[1] + jnp.where(inside, update * update, 0.0),
            )

        nothing = jnp.zeros((BLOCK, LANES), jnp.float32)
        weights, updates = lax.fori_loop(
            begin // MARGIN, (finish + MARGIN - 1) // MARGIN, add, (nothing, nothing)
        )
        row = jnp.where(lane == s, jnp.sum(weights, axis=(0, 1), keepdims=True), row)
        return jnp.where(lane == s + segs, jnp.sum(updates, axis=(0, 1), keepdims=True), row)

    part[...] = lax.fori_loop(first, end, tensor, jnp.zeros((1, LANES), jnp.float32))

    start = count - MARGIN
    top = start // LANES
    lanes = start & (LANES - 1)
    for a in range(4):
        head[a] = state[a, PAD : PAD + BLOCK, :]
        tail[a] = moved(
            state[a, pl.ds(PAD + top, BLOCK), :], state[a, pl.ds(PAD + top + 1, BLOCK), :], lanes
        )


def exchange_kernel(axis, n, part, tail, head, sums, left_rim, right_rim, slots, send, receive, rim_send, rim_receive):
    me = lax.axis_index(axis)
    right = lax.rem(me + 1, n)
    left = lax.rem(me + n - 1, n)
    barrier = pltpu.get_barrier_semaphore()

    def greet(k, carry):
        pl.semaphore_signal(barrier, inc=1, device_id=(lax.rem(me + k, n),), device_id_type=MESH)
        return carry

    lax.fori_loop(1, n, greet, 0)
    slots[me] = part[...]
    pl.semaphore_wait(barrier, n - 1)

    def tell(k):
        return pltpu.make_async_remote_copy(
            src_ref=part,
            dst_ref=slots.at[me],
            send_sem=send.at[k],
            recv_sem=receive.at[k],
            device_id=(lax.rem(me + k, n),),
            device_id_type=MESH,
        )

    def hear(k):
        source = lax.rem(me + n - k, n)
        return pltpu.make_async_remote_copy(
            src_ref=part,
            dst_ref=slots.at[source],
            send_sem=send.at[k],
            recv_sem=receive.at[k],
            device_id=(source,),
            device_id_type=MESH,
        )

    onward = pltpu.make_async_remote_copy(
        src_ref=tail,
        dst_ref=left_rim,
        send_sem=rim_send.at[0],
        recv_sem=rim_receive.at[0],
        device_id=(right,),
        device_id_type=MESH,
    )
    back = pltpu.make_async_remote_copy(
        src_ref=head,
        dst_ref=right_rim,
        send_sem=rim_send.at[1],
        recv_sem=rim_receive.at[1],
        device_id=(left,),
        device_id_type=MESH,
    )

    def start(k, carry):
        tell(k).start()
        return carry

    def finish(k, carry):
        tell(k).wait_send()
        hear(k).wait_recv()
        return carry

    lax.fori_loop(1, n, start, 0)
    onward.start()
    back.start()
    lax.fori_loop(1, n, finish, 0)
    sums[...] = jnp.sum(slots[...], axis=0)
    onward.wait()
    back.wait()


def place_kernel(axis, old_ref, new_ref, seg_ref, state, sums, left_rim, right_rim, w_out, m_out, v_out, w_buf, u_buf, m_buf, v_buf, before, after, sems):
    rows = w_buf.shape[0]
    blocks = rows // BLOCK
    me = lax.axis_index(axis)
    old_low = old_ref[me]
    old_count = old_ref[me + 1] - old_low
    new_low = new_ref[me]
    new_high = new_ref[me + 1]
    new_count = new_high - new_low
    shift = new_low - old_low
    top = shift // LANES
    lanes = shift & (LANES - 1)
    flat = flat_ids()
    targets = (w_buf, u_buf, m_buf, v_buf)

    for a in range(4):
        before[a, 0:BLOCK, :] = left_rim[a]
        before[a, BLOCK:EDGE, :] = state[a, PAD : PAD + EDGE - BLOCK, :]
        after[a, PAD : PAD + BLOCK, :] = right_rim[a]
        targets[a][0:BLOCK, :] = moved(
            before[a, pl.ds(BLOCK + top, BLOCK), :], before[a, pl.ds(BLOCK + top + 1, BLOCK), :], lanes
        )

    def own(a, b):
        there = b * BLOCK + PAD + top
        return moved(state[a, pl.ds(there, BLOCK), :], state[a, pl.ds(there + 1, BLOCK), :], lanes)

    def inner(b, carry):
        here = pl.multiple_of(b * BLOCK, BLOCK)
        for a in range(4):
            targets[a][pl.ds(here, BLOCK), :] = own(a, b)
        return carry

    lax.fori_loop(1, blocks - 3, inner, 0)

    for b in range(blocks - 3, blocks):
        offset = b * MARGIN + shift - old_count
        row = jnp.clip(offset // LANES, -PAD, PAD - 7) + PAD
        side = offset & (LANES - 1)
        index = flat + b * MARGIN
        beyond = index + shift >= old_count
        live = index < new_count
        for a in range(4):
            rim = moved(after[a, pl.ds(row, BLOCK), :], after[a, pl.ds(row + 1, BLOCK), :], side)
            value = jnp.where(beyond, rim, own(a, b))
            targets[a][b * BLOCK : (b + 1) * BLOCK, :] = jnp.where(live, value, 0.0)

    m_copy = pltpu.make_async_copy(m_buf, m_out, sems.at[1])
    v_copy = pltpu.make_async_copy(v_buf, v_out, sems.at[2])
    m_copy.start()
    v_copy.start()

    segs = seg_ref.shape[0]
    total = sums[...]
    other = pltpu.roll(total, LANES - segs, 1)
    rate = LEARN * (jnp.sqrt(total) / (jnp.sqrt(other) + EPSILON))
    lane = lane_ids(1)
    first, end = overlapping(seg_ref, new_low, new_high)

    def tensor(s, carry):
        begin, finish = span_of(seg_ref, s, new_low, new_count)
        factor = jnp.sum(jnp.where(lane == s, rate, 0.0), axis=1, keepdims=True)

        def apply(b, inner_carry):
            here = pl.ds(pl.multiple_of(b * BLOCK, BLOCK), BLOCK)
            index = flat + b * MARGIN
            inside = (index >= begin) & (index < finish)
            weight = w_buf[here, :]
            w_buf[here, :] = jnp.where(inside, weight - factor * u_buf[here, :], weight)
            return inner_carry

        return lax.fori_loop(begin // MARGIN, (finish + MARGIN - 1) // MARGIN, apply, carry)

    lax.fori_loop(first, end, tensor, 0)
    w_copy = pltpu.make_async_copy(w_buf, w_out, sems.at[0])
    w_copy.start()
    m_copy.wait()
    v_copy.wait()
    w_copy.wait()


def spec(space):
    return pl.BlockSpec(memory_space=space)


def shards(axis, n, params, first_moment, second_moment, grads, old_bounds, new_bounds, seg_start):
    cap = params.shape[0]
    rows = cap // LANES
    f32 = jnp.float32
    flat = [x.reshape(rows, LANES) for x in (params, first_moment, second_moment, grads)]
    rim = jax.ShapeDtypeStruct((4, BLOCK, LANES), f32)
    line = jax.ShapeDtypeStruct((1, LANES), f32)
    smem, vmem, hbm = spec(pltpu.SMEM), spec(pltpu.VMEM), spec(pl.ANY)
    state, part, tail, head = pl.pallas_call(
        functools.partial(update_kernel, axis),
        name="update",
        out_shape=(jax.ShapeDtypeStruct((4, rows + 2 * PAD, LANES), f32), line, rim, rim),
        in_specs=[smem, smem, hbm, hbm, hbm, hbm],
        out_specs=(vmem,) * 4,
        scratch_shapes=[
            pltpu.VMEM((rows, LANES), f32),
            pltpu.VMEM((rows, LANES), f32),
            pltpu.VMEM((rows, LANES), grads.dtype),
            pltpu.SemaphoreType.DMA((4, 4)),
        ],
        compiler_params=pltpu.CompilerParams(vmem_limit_bytes=VMEM_LIMIT),
    )(old_bounds, seg_start, *flat)
    sums, left_rim, right_rim = pl.pallas_call(
        functools.partial(exchange_kernel, axis, n),
        name="exchange",
        out_shape=(line, rim, rim),
        in_specs=[vmem] * 3,
        out_specs=(vmem,) * 3,
        scratch_shapes=[
            pltpu.VMEM((n, 1, LANES), f32),
            pltpu.SemaphoreType.DMA((n,)),
            pltpu.SemaphoreType.DMA((n,)),
            pltpu.SemaphoreType.DMA((2,)),
            pltpu.SemaphoreType.DMA((2,)),
        ],
        compiler_params=pltpu.CompilerParams(
            collective_id=0, has_side_effects=True, vmem_limit_bytes=VMEM_LIMIT
        ),
    )(part, tail, head)
    whole = jax.ShapeDtypeStruct((rows, LANES), f32)
    outs = pl.pallas_call(
        functools.partial(place_kernel, axis),
        name="place",
        out_shape=(whole,) * 3,
        in_specs=[smem, smem, smem, vmem, vmem, vmem, vmem],
        out_specs=(hbm,) * 3,
        scratch_shapes=[pltpu.VMEM((rows, LANES), f32)] * 4
        + [pltpu.VMEM((4, EDGE, LANES), f32)] * 2
        + [pltpu.SemaphoreType.DMA((3,))],
        compiler_params=pltpu.CompilerParams(vmem_limit_bytes=VMEM_LIMIT),
    )(old_bounds, new_bounds, seg_start, state, sums, left_rim, right_rim)
    return tuple(x.reshape(cap) for x in outs)


def solution(mesh):
    (axis,) = mesh.axis_names
    n = mesh.shape[axis]
    placed = (P(axis), P(axis), P(axis), P(axis), P(), P(), P())
    return jax.shard_map(
        functools.partial(shards, axis, n),
        mesh=mesh,
        in_specs=placed,
        out_specs=(P(axis), P(axis), P(axis)),
        check_vma=False,
    )
```

```python
import functools

import jax
import jax.numpy as jnp
from jax import lax
from jax.experimental import pallas as pl
from jax.experimental.pallas import tpu as pltpu
from jax.sharding import PartitionSpec as P

MARGIN = 4096
LANES = 128
BLOCK = MARGIN // LANES
PAD = BLOCK + 8
EDGE = 2 * PAD + BLOCK


BETA_ONE = 0.9
BETA_TWO = 0.999
CORR_ONE = 1.0 - 0.9**10
CORR_TWO = 1.0 - 0.999**10
DECAY = 0.01
LEARN = 0.1
EPSILON = 1e-06

MESH = pl.DeviceIdType.MESH
VMEM_LIMIT = 16 * 1024 * 1024


def lane_ids(rows=BLOCK):
    return lax.broadcasted_iota(jnp.int32, (rows, LANES), 1)


def flat_ids():
    return lax.broadcasted_iota(jnp.int32, (BLOCK, LANES), 0) * LANES + lane_ids()


def moved(first, second, lanes):
    picked = jnp.where(lane_ids() >= lanes, first, second)
    return pltpu.roll(picked, (LANES - lanes) & (LANES - 1), 1)


def overlapping(seg_ref, low, high):
    def step(s, carry):
        first, end = carry
        start = seg_ref[s]
        return (first + (start <= low).astype(jnp.int32), end + (start < high).astype(jnp.int32))

    first, end = lax.fori_loop(0, seg_ref.shape[0], step, (jnp.int32(-1), jnp.int32(0)), unroll=8)
    return first, end


def span_of(seg_ref, s, low, count):
    segs = seg_ref.shape[0]
    begin = jnp.maximum(seg_ref[s] - low, 0)
    after = seg_ref[jnp.minimum(s + 1, segs - 1)] - low
    finish = jnp.where(s + 1 < segs, jnp.minimum(after, count), count)
    return begin, finish


def fetched(tables, refs, sems):
    copies = [pltpu.make_async_copy(t, r, sems.at[i]) for i, (t, r) in enumerate(zip(tables, refs))]
    for copy in copies:
        copy.start()
    return copies


def update_kernel(axis, old_hbm, seg_hbm, w_hbm, m_hbm, v_hbm, g_hbm, state, part, tail, head, m_buf, v_buf, g_buf, old_ref, seg_ref, sems, table_sems):
    rows = m_buf.shape[0]
    tables = fetched((old_hbm, seg_hbm), (old_ref, seg_ref), table_sems)
    blocks = rows // BLOCK
    step_blocks = -(-blocks // sems.shape[1])
    chunks = [(b, min(b + step_blocks, blocks)) for b in range(0, blocks, step_blocks)]
    copies = []
    for c, (b0, b1) in enumerate(chunks):
        window = pl.ds(b0 * BLOCK, (b1 - b0) * BLOCK)
        placed = state.at[0, pl.ds(PAD + b0 * BLOCK, (b1 - b0) * BLOCK)]
        group = [
            pltpu.make_async_copy(w_hbm.at[window], placed, sems.at[0, c]),
            pltpu.make_async_copy(m_hbm.at[window], m_buf.at[window], sems.at[1, c]),
            pltpu.make_async_copy(v_hbm.at[window], v_buf.at[window], sems.at[2, c]),
            pltpu.make_async_copy(g_hbm.at[window], g_buf.at[window], sems.at[3, c]),
        ]
        for copy in group:
            copy.start()
        copies.append(group)

    for copy in tables:
        copy.wait()
    me = lax.axis_index(axis)
    low = old_ref[me]
    high = old_ref[me + 1]
    count = high - low
    first, end = overlapping(seg_ref, low, high)

    def advance(b, carry):
        here = pl.multiple_of(b * BLOCK, BLOCK)
        there = pl.multiple_of(b * BLOCK + PAD, 8)
        gradient = g_buf[pl.ds(here, BLOCK), :].astype(jnp.float32)
        weight = state[0, pl.ds(there, BLOCK), :]
        moment = BETA_ONE * m_buf[pl.ds(here, BLOCK), :] + (1.0 - BETA_ONE) * gradient
        second = BETA_TWO * v_buf[pl.ds(here, BLOCK), :] + (1.0 - BETA_TWO) * gradient * gradient
        scaled = moment * (1.0 / CORR_ONE)
        update = scaled / (jnp.sqrt(second * (1.0 / CORR_TWO)) + EPSILON) + DECAY * weight
        state[1, pl.ds(there, BLOCK), :] = update
        state[2, pl.ds(there, BLOCK), :] = moment
        state[3, pl.ds(there, BLOCK), :] = second
        return carry

    for (b0, b1), group in zip(chunks, copies):
        for copy in group:
            copy.wait()
        lax.fori_loop(b0, b1, advance, 0)

    flat = flat_ids()
    lane = lane_ids(1)
    segs = seg_ref.shape[0]

    def tensor(s, row):
        begin, finish = span_of(seg_ref, s, low, count)

        def add(b, carry):
            there = pl.multiple_of(b * BLOCK + PAD, 8)
            index = flat + b * MARGIN
            inside = (index >= begin) & (index < finish)
            weight = state[0, pl.ds(there, BLOCK), :]
            update = state[1, pl.ds(there, BLOCK), :]
            return (
                carry[0] + jnp.where(inside, weight * weight, 0.0),
                carry[1] + jnp.where(inside, update * update, 0.0),
            )

        nothing = jnp.zeros((BLOCK, LANES), jnp.float32)
        weights, updates = lax.fori_loop(
            begin // MARGIN, (finish + MARGIN - 1) // MARGIN, add, (nothing, nothing)
        )
        row = jnp.where(lane == s, jnp.sum(weights, axis=(0, 1), keepdims=True), row)
        return jnp.where(lane == s + segs, jnp.sum(updates, axis=(0, 1), keepdims=True), row)

    part[...] = lax.fori_loop(first, end, tensor, jnp.zeros((1, LANES), jnp.float32))

    start = count - MARGIN
    top = start // LANES
    lanes = start & (LANES - 1)
    for a in range(4):
        head[a] = state[a, PAD : PAD + BLOCK, :]
        tail[a] = moved(
            state[a, pl.ds(PAD + top, BLOCK), :], state[a, pl.ds(PAD + top + 1, BLOCK), :], lanes
        )


def exchange_kernel(axis, n, part, tail, head, sums, left_rim, right_rim, slots, send, receive, rim_send, rim_receive):
    me = lax.axis_index(axis)
    right = lax.rem(me + 1, n)
    left = lax.rem(me + n - 1, n)
    barrier = pltpu.get_barrier_semaphore()

    def greet(k, carry):
        pl.semaphore_signal(barrier, inc=1, device_id=(lax.rem(me + k, n),), device_id_type=MESH)
        return carry

    lax.fori_loop(1, n, greet, 0)
    slots[me] = part[...]
    pl.semaphore_wait(barrier, n - 1)

    def tell(k):
        return pltpu.make_async_remote_copy(
            src_ref=part,
            dst_ref=slots.at[me],
            send_sem=send.at[k],
            recv_sem=receive.at[k],
            device_id=(lax.rem(me + k, n),),
            device_id_type=MESH,
        )

    def hear(k):
        source = lax.rem(me + n - k, n)
        return pltpu.make_async_remote_copy(
            src_ref=part,
            dst_ref=slots.at[source],
            send_sem=send.at[k],
            recv_sem=receive.at[k],
            device_id=(source,),
            device_id_type=MESH,
        )

    onward = pltpu.make_async_remote_copy(
        src_ref=tail,
        dst_ref=left_rim,
        send_sem=rim_send.at[0],
        recv_sem=rim_receive.at[0],
        device_id=(right,),
        device_id_type=MESH,
    )
    back = pltpu.make_async_remote_copy(
        src_ref=head,
        dst_ref=right_rim,
        send_sem=rim_send.at[1],
        recv_sem=rim_receive.at[1],
        device_id=(left,),
        device_id_type=MESH,
    )

    def start(k, carry):
        tell(k).start()
        return carry

    def finish(k, carry):
        tell(k).wait_send()
        hear(k).wait_recv()
        return carry

    lax.fori_loop(1, n, start, 0)
    onward.start()
    back.start()
    lax.fori_loop(1, n, finish, 0)
    sums[...] = jnp.sum(slots[...], axis=0)
    onward.wait()
    back.wait()


def place_kernel(axis, old_hbm, new_hbm, seg_hbm, state, sums, left_rim, right_rim, w_out, m_out, v_out, w_buf, u_buf, m_buf, v_buf, before, after, old_ref, new_ref, seg_ref, sems, table_sems):
    tables = fetched((old_hbm, new_hbm, seg_hbm), (old_ref, new_ref, seg_ref), table_sems)
    rows = w_buf.shape[0]
    blocks = rows // BLOCK
    for a in range(4):
        before[a, 0:BLOCK, :] = left_rim[a]
        before[a, BLOCK:EDGE, :] = state[a, PAD : PAD + EDGE - BLOCK, :]
        after[a, PAD : PAD + BLOCK, :] = right_rim[a]
    for copy in tables:
        copy.wait()
    me = lax.axis_index(axis)
    old_low = old_ref[me]
    old_count = old_ref[me + 1] - old_low
    new_low = new_ref[me]
    new_high = new_ref[me + 1]
    new_count = new_high - new_low
    shift = new_low - old_low
    top = shift // LANES
    lanes = shift & (LANES - 1)
    flat = flat_ids()
    targets = (w_buf, u_buf, m_buf, v_buf)

    for a in range(4):
        targets[a][0:BLOCK, :] = moved(
            before[a, pl.ds(BLOCK + top, BLOCK), :], before[a, pl.ds(BLOCK + top + 1, BLOCK), :], lanes
        )

    def own(a, b):
        there = b * BLOCK + PAD + top
        return moved(state[a, pl.ds(there, BLOCK), :], state[a, pl.ds(there + 1, BLOCK), :], lanes)

    def inner(b, carry):
        here = pl.multiple_of(b * BLOCK, BLOCK)
        for a in range(4):
            targets[a][pl.ds(here, BLOCK), :] = own(a, b)
        return carry

    lax.fori_loop(1, blocks - 3, inner, 0)

    for b in range(blocks - 3, blocks):
        offset = b * MARGIN + shift - old_count
        row = jnp.clip(offset // LANES, -PAD, PAD - 7) + PAD
        side = offset & (LANES - 1)
        index = flat + b * MARGIN
        beyond = index + shift >= old_count
        live = index < new_count
        for a in range(4):
            rim = moved(after[a, pl.ds(row, BLOCK), :], after[a, pl.ds(row + 1, BLOCK), :], side)
            value = jnp.where(beyond, rim, own(a, b))
            targets[a][b * BLOCK : (b + 1) * BLOCK, :] = jnp.where(live, value, 0.0)

    m_copy = pltpu.make_async_copy(m_buf, m_out, sems.at[1])
    v_copy = pltpu.make_async_copy(v_buf, v_out, sems.at[2])
    m_copy.start()
    v_copy.start()

    segs = seg_ref.shape[0]
    total = sums[...]
    other = pltpu.roll(total, LANES - segs, 1)
    rate = LEARN * (jnp.sqrt(total) / (jnp.sqrt(other) + EPSILON))
    lane = lane_ids(1)
    first, end = overlapping(seg_ref, new_low, new_high)

    def tensor(s, carry):
        begin, finish = span_of(seg_ref, s, new_low, new_count)
        factor = jnp.sum(jnp.where(lane == s, rate, 0.0), axis=1, keepdims=True)

        def apply(b, inner_carry):
            here = pl.ds(pl.multiple_of(b * BLOCK, BLOCK), BLOCK)
            index = flat + b * MARGIN
            inside = (index >= begin) & (index < finish)
            weight = w_buf[here, :]
            w_buf[here, :] = jnp.where(inside, weight - factor * u_buf[here, :], weight)
            return inner_carry

        return lax.fori_loop(begin // MARGIN, (finish + MARGIN - 1) // MARGIN, apply, carry)

    lax.fori_loop(first, end, tensor, 0)
    w_copy = pltpu.make_async_copy(w_buf, w_out, sems.at[0])
    w_copy.start()
    m_copy.wait()
    v_copy.wait()
    w_copy.wait()


def spec(space):
    return pl.BlockSpec(memory_space=space)


def shards(axis, n, params, first_moment, second_moment, grads, old_bounds, new_bounds, seg_start):
    cap = params.shape[0]
    rows = cap // LANES
    f32 = jnp.float32
    flat = [x.reshape(rows, LANES) for x in (params, first_moment, second_moment, grads)]
    old_bounds, new_bounds, seg_start, *flat = (
        pltpu.with_memory_space_constraint(x, pltpu.HBM) for x in (old_bounds, new_bounds, seg_start, *flat)
    )
    rim = jax.ShapeDtypeStruct((4, BLOCK, LANES), f32)
    line = jax.ShapeDtypeStruct((1, LANES), f32)
    vmem, hbm = spec(pltpu.VMEM), spec(pltpu.HBM)
    bounds = pltpu.SMEM(old_bounds.shape, jnp.int32)
    starts = pltpu.SMEM(seg_start.shape, jnp.int32)
    state, part, tail, head = pl.pallas_call(
        functools.partial(update_kernel, axis),
        name="update",
        out_shape=(jax.ShapeDtypeStruct((4, rows + 2 * PAD, LANES), f32), line, rim, rim),
        in_specs=[hbm] * 6,
        out_specs=(vmem,) * 4,
        scratch_shapes=[
            pltpu.VMEM((rows, LANES), f32),
            pltpu.VMEM((rows, LANES), f32),
            pltpu.VMEM((rows, LANES), grads.dtype),
            bounds,
            starts,
            pltpu.SemaphoreType.DMA((4, 4)),
            pltpu.SemaphoreType.DMA((2,)),
        ],
        compiler_params=pltpu.CompilerParams(vmem_limit_bytes=VMEM_LIMIT),
    )(old_bounds, seg_start, *flat)
    sums, left_rim, right_rim = pl.pallas_call(
        functools.partial(exchange_kernel, axis, n),
        name="exchange",
        out_shape=(line, rim, rim),
        in_specs=[vmem] * 3,
        out_specs=(vmem,) * 3,
        scratch_shapes=[
            pltpu.VMEM((n, 1, LANES), f32),
            pltpu.SemaphoreType.DMA((n,)),
            pltpu.SemaphoreType.DMA((n,)),
            pltpu.SemaphoreType.DMA((2,)),
            pltpu.SemaphoreType.DMA((2,)),
        ],
        compiler_params=pltpu.CompilerParams(
            collective_id=0, has_side_effects=True, vmem_limit_bytes=VMEM_LIMIT
        ),
    )(part, tail, head)
    whole = jax.ShapeDtypeStruct((rows, LANES), f32)
    outs = pl.pallas_call(
        functools.partial(place_kernel, axis),
        name="place",
        out_shape=(whole,) * 3,
        in_specs=[hbm, hbm, hbm, vmem, vmem, vmem, vmem],
        out_specs=(hbm,) * 3,
        scratch_shapes=[pltpu.VMEM((rows, LANES), f32)] * 4
        + [pltpu.VMEM((4, EDGE, LANES), f32)] * 2
        + [bounds, bounds, starts, pltpu.SemaphoreType.DMA((3,)), pltpu.SemaphoreType.DMA((3,))],
        compiler_params=pltpu.CompilerParams(vmem_limit_bytes=VMEM_LIMIT),
    )(old_bounds, new_bounds, seg_start, state, sums, left_rim, right_rim)
    return tuple(x.reshape(cap) for x in outs)


def solution(mesh):
    (axis,) = mesh.axis_names
    n = mesh.shape[axis]
    placed = (P(axis), P(axis), P(axis), P(axis), P(), P(), P())
    return jax.shard_map(
        functools.partial(shards, axis, n),
        mesh=mesh,
        in_specs=placed,
        out_specs=(P(axis), P(axis), P(axis)),
        check_vma=False,
    )
```

```python
import functools

import jax
import jax.numpy as jnp
from jax import lax
from jax.experimental import pallas as pl
from jax.experimental.pallas import tpu as pltpu
from jax.sharding import PartitionSpec as P

MARGIN = 4096
LANES = 128
BLOCK = MARGIN // LANES
HALF = 64
HALF_BITS = 6
LANE_BITS = 7
PAD = BLOCK + 8
EDGE = 2 * PAD + BLOCK


BETA_ONE = 0.9
BETA_TWO = 0.999
CORR_ONE = 1.0 - 0.9**10
CORR_TWO = 1.0 - 0.999**10
DECAY = 0.01
LEARN = 0.1
EPSILON = 1e-06

MESH = pl.DeviceIdType.MESH
VMEM_LIMIT = 16 * 1024 * 1024


def lane_ids(rows=BLOCK):
    return lax.broadcasted_iota(jnp.int32, (rows, LANES), 1)


def flat_ids():
    return lax.broadcasted_iota(jnp.int32, (BLOCK, LANES), 0) * LANES + lane_ids()


def moved(first, second, lanes):
    picked = jnp.where(lane_ids() >= lanes, first, second)
    return pltpu.roll(picked, (LANES - lanes) & (LANES - 1), 1)


def overlapping(seg_ref, low, high):
    def step(s, carry):
        first, end = carry
        start = seg_ref[s]
        return (first + (start <= low).astype(jnp.int32), end + (start < high).astype(jnp.int32))

    first, end = lax.fori_loop(0, seg_ref.shape[0], step, (jnp.int32(-1), jnp.int32(0)), unroll=8)
    return first, end


def span_of(seg_ref, s, low, count):
    segs = seg_ref.shape[0]
    begin = jnp.maximum(seg_ref[s] - low, 0)
    after = seg_ref[jnp.minimum(s + 1, segs - 1)] - low
    finish = jnp.where(s + 1 < segs, jnp.minimum(after, count), count)
    return begin, finish


def fetched(tables, refs, sems):
    copies = [pltpu.make_async_copy(t, r, sems.at[i]) for i, (t, r) in enumerate(zip(tables, refs))]
    for copy in copies:
        copy.start()
    return copies


def step_kernel(
    axis, n, old_hbm, new_hbm, seg_hbm, w_hbm, m_hbm, v_hbm, g_hbm, placed, sums,
    state, m_buf, v_buf, g_buf, squares, member, begins, ends, part, tail, head, left_rim, right_rim,
    before, after, slots, old_ref, new_ref, seg_ref, sems, table_sems, send, receive, rim_send, rim_receive,
):
    rows = m_buf.shape[0]
    blocks = rows // BLOCK
    segs = seg_ref.shape[0]
    me = lax.axis_index(axis)
    right = lax.rem(me + 1, n)
    left = lax.rem(me + n - 1, n)
    tables = fetched((old_hbm, new_hbm, seg_hbm), (old_ref, new_ref, seg_ref), table_sems)
    step_blocks = -(-blocks // sems.shape[1])
    chunks = [(b, min(b + step_blocks, blocks)) for b in range(0, blocks, step_blocks)]
    copies = []
    for c, (b0, b1) in enumerate(chunks):
        window = pl.ds(b0 * BLOCK, (b1 - b0) * BLOCK)
        inside = state.at[0, pl.ds(PAD + b0 * BLOCK, (b1 - b0) * BLOCK)]
        group = [
            pltpu.make_async_copy(w_hbm.at[window], inside, sems.at[0, c]),
            pltpu.make_async_copy(m_hbm.at[window], m_buf.at[window], sems.at[1, c]),
            pltpu.make_async_copy(v_hbm.at[window], v_buf.at[window], sems.at[2, c]),
            pltpu.make_async_copy(g_hbm.at[window], g_buf.at[window], sems.at[3, c]),
        ]
        for copy in group:
            copy.start()
        copies.append(group)

    barrier = pltpu.get_barrier_semaphore()

    def greet(k, carry):
        pl.semaphore_signal(barrier, inc=1, device_id=(lax.rem(me + k, n),), device_id_type=MESH)
        return carry

    lax.fori_loop(1, n, greet, 0)

    for copy in tables:
        copy.wait()
    low = old_ref[me]
    count = old_ref[me + 1] - low
    new_low = new_ref[me]
    new_count = new_ref[me + 1] - new_low
    shift = new_low - low
    phase = (-low) & (HALF - 1)

    def bound(s, carry):
        value = (seg_ref[s] - low - phase) >> HALF_BITS
        begins[pl.ds(s, 1), :] = jnp.full((1, LANES), value, jnp.int32)
        following = (seg_ref[jnp.minimum(s + 1, segs - 1)] - low - phase) >> HALF_BITS
        following = jnp.where(s + 1 < segs, following, 4 * rows)
        ends[pl.ds(s, 1), :] = jnp.full((1, LANES), following, jnp.int32)
        return carry

    lax.fori_loop(0, segs, bound, 0, unroll=8)
    padded = member.shape[1]
    spot = lane_ids(segs)
    first_half = begins[...]
    past_half = ends[...]
    for group in range(3):
        for tile in range(padded // LANES):
            half = 2 * (spot + tile * LANES) - 1 + group
            mask = (half >= first_half) & (half < past_half)
            member[group * segs : (group + 1) * segs, tile * LANES : (tile + 1) * LANES] = jnp.where(
                mask, 1.0, 0.0
            ).astype(jnp.bfloat16)
    squares[rows:padded, :] = jnp.zeros((padded - rows, 4 * LANES), jnp.bfloat16)

    flat = flat_ids()

    def advance(b, carry):
        here = pl.multiple_of(b * BLOCK, BLOCK)
        there = pl.multiple_of(b * BLOCK + PAD, 8)
        gradient = g_buf[pl.ds(here, BLOCK), :].astype(jnp.float32)
        weight = state[0, pl.ds(there, BLOCK), :]
        moment = BETA_ONE * m_buf[pl.ds(here, BLOCK), :] + (1.0 - BETA_ONE) * gradient
        second = BETA_TWO * v_buf[pl.ds(here, BLOCK), :] + (1.0 - BETA_TWO) * gradient * gradient
        scaled = moment * (1.0 / CORR_ONE)
        update = scaled / (jnp.sqrt(second * (1.0 / CORR_TWO)) + EPSILON) + DECAY * weight
        state[1, pl.ds(there, BLOCK), :] = update
        state[2, pl.ds(there, BLOCK), :] = moment
        state[3, pl.ds(there, BLOCK), :] = second
        live = flat + b * MARGIN < count
        for i, value in enumerate((weight, update)):
            square = jnp.where(live, value * value, 0.0)
            coarse = square.astype(jnp.bfloat16)
            fine = (square - coarse.astype(jnp.float32)).astype(jnp.bfloat16)
            squares[pl.ds(here, BLOCK), i * LANES : (i + 1) * LANES] = coarse
            squares[pl.ds(here, BLOCK), (i + 2) * LANES : (i + 3) * LANES] = fine
        return carry

    for (b0, b1), group in zip(chunks, copies):
        for copy in group:
            copy.wait()
        lax.fori_loop(b0, b1, advance, 0)

    start = count - MARGIN
    start_row = start >> LANE_BITS
    start_lane = start & (LANES - 1)
    for a in range(4):
        head[a] = state[a, PAD : PAD + BLOCK, :]
        tail[a] = moved(
            state[a, pl.ds(PAD + start_row, BLOCK), :],
            state[a, pl.ds(PAD + start_row + 1, BLOCK), :],
            start_lane,
        )

    product = jnp.dot(member[...], squares[...], preferred_element_type=jnp.float32)
    product = product[:, : 2 * LANES] + product[:, 2 * LANES :]
    line = lax.broadcasted_iota(jnp.int32, (segs, LANES), 0)
    row = jnp.zeros((segs, LANES), jnp.float32)
    for i in range(2):
        columns = slice(i * LANES, (i + 1) * LANES)
        mixed = jnp.where(
            spot < phase,
            product[0:segs, columns],
            jnp.where(
                spot < phase + HALF, product[segs : 2 * segs, columns], product[2 * segs : 3 * segs, columns]
            ),
        )
        row = jnp.where(spot == line + i * segs, jnp.sum(mixed, axis=1, keepdims=True), row)
    part[...] = jnp.sum(row, axis=0, keepdims=True)
    slots[me] = part[...]
    pl.semaphore_wait(barrier, n - 1)

    def tell(k):
        return pltpu.make_async_remote_copy(
            src_ref=part,
            dst_ref=slots.at[me],
            send_sem=send.at[k],
            recv_sem=receive.at[k],
            device_id=(lax.rem(me + k, n),),
            device_id_type=MESH,
        )

    def hear(k):
        source = lax.rem(me + n - k, n)
        return pltpu.make_async_remote_copy(
            src_ref=part,
            dst_ref=slots.at[source],
            send_sem=send.at[k],
            recv_sem=receive.at[k],
            device_id=(source,),
            device_id_type=MESH,
        )

    onward = pltpu.make_async_remote_copy(
        src_ref=tail,
        dst_ref=left_rim,
        send_sem=rim_send.at[0],
        recv_sem=rim_receive.at[0],
        device_id=(right,),
        device_id_type=MESH,
    )
    back = pltpu.make_async_remote_copy(
        src_ref=head,
        dst_ref=right_rim,
        send_sem=rim_send.at[1],
        recv_sem=rim_receive.at[1],
        device_id=(left,),
        device_id_type=MESH,
    )

    def begin(k, carry):
        tell(k).start()
        return carry

    def finish(k, carry):
        tell(k).wait_send()
        hear(k).wait_recv()
        return carry

    lax.fori_loop(1, n, begin, 0)
    onward.start()
    back.start()

    top = shift >> LANE_BITS
    lanes = shift & (LANES - 1)

    def own(a, b):
        there = b * BLOCK + PAD + top
        return moved(state[a, pl.ds(there, BLOCK), :], state[a, pl.ds(there + 1, BLOCK), :], lanes)

    def inner(b, carry):
        here = pl.multiple_of(b * BLOCK, BLOCK)
        for a in range(4):
            placed[a, pl.ds(here, BLOCK), :] = own(a, b)
        return carry

    lax.fori_loop(1, blocks - 3, inner, 0)
    for a in range(4):
        before[a, BLOCK:EDGE, :] = state[a, PAD : PAD + EDGE - BLOCK, :]
    onward.wait()
    back.wait()
    for a in range(4):
        before[a, 0:BLOCK, :] = left_rim[a]
        after[a, PAD : PAD + BLOCK, :] = right_rim[a]
    for a in range(4):
        placed[a, 0:BLOCK, :] = moved(
            before[a, pl.ds(BLOCK + top, BLOCK), :], before[a, pl.ds(BLOCK + top + 1, BLOCK), :], lanes
        )

    for b in range(blocks - 3, blocks):
        offset = b * MARGIN + shift - count
        near = jnp.clip(offset >> LANE_BITS, -PAD, PAD - 7) + PAD
        side = offset & (LANES - 1)
        index = flat + b * MARGIN
        beyond = index + shift >= count
        live = index < new_count
        for a in range(4):
            rim = moved(after[a, pl.ds(near, BLOCK), :], after[a, pl.ds(near + 1, BLOCK), :], side)
            value = jnp.where(beyond, rim, own(a, b))
            placed[a, b * BLOCK : (b + 1) * BLOCK, :] = jnp.where(live, value, 0.0)

    lax.fori_loop(1, n, finish, 0)
    sums[...] = jnp.sum(slots[...], axis=0)


def apply_kernel(axis, new_hbm, seg_hbm, placed, sums, w_out, m_out, v_out, w_buf, new_ref, seg_ref, sems, table_sems):
    tables = fetched((new_hbm, seg_hbm), (new_ref, seg_ref), table_sems)
    m_copy = pltpu.make_async_copy(placed.at[2], m_out, sems.at[1])
    v_copy = pltpu.make_async_copy(placed.at[3], v_out, sems.at[2])
    m_copy.start()
    v_copy.start()
    rows = w_buf.shape[0]
    w_buf[...] = placed[0]
    segs = seg_ref.shape[0]
    total = sums[...]
    other = pltpu.roll(total, LANES - segs, 1)
    rate = LEARN * (jnp.sqrt(total) / (jnp.sqrt(other) + EPSILON))
    lane = lane_ids(1)
    flat = flat_ids()
    for copy in tables:
        copy.wait()
    me = lax.axis_index(axis)
    new_low = new_ref[me]
    new_high = new_ref[me + 1]
    new_count = new_high - new_low
    first, end = overlapping(seg_ref, new_low, new_high)

    def tensor(s, carry):
        begin, finish = span_of(seg_ref, s, new_low, new_count)
        factor = jnp.sum(jnp.where(lane == s, rate, 0.0), axis=1, keepdims=True)

        def apply(b, inner_carry):
            here = pl.ds(pl.multiple_of(b * BLOCK, BLOCK), BLOCK)
            index = flat + b * MARGIN
            inside = (index >= begin) & (index < finish)
            weight = w_buf[here, :]
            w_buf[here, :] = jnp.where(inside, weight - factor * placed[1, here, :], weight)
            return inner_carry

        return lax.fori_loop(begin // MARGIN, (finish + MARGIN - 1) // MARGIN, apply, carry)

    lax.fori_loop(first, end, tensor, 0)
    w_copy = pltpu.make_async_copy(w_buf, w_out, sems.at[0])
    w_copy.start()
    m_copy.wait()
    v_copy.wait()
    w_copy.wait()


def spec(space):
    return pl.BlockSpec(memory_space=space)


def shards(axis, n, params, first_moment, second_moment, grads, old_bounds, new_bounds, seg_start):
    cap = params.shape[0]
    rows = cap // LANES
    f32 = jnp.float32
    flat = [x.reshape(rows, LANES) for x in (params, first_moment, second_moment, grads)]
    old_bounds, new_bounds, seg_start, *flat = (
        pltpu.with_memory_space_constraint(x, pltpu.HBM) for x in (old_bounds, new_bounds, seg_start, *flat)
    )
    segs = seg_start.shape[0]
    padded = -(-rows // 256) * 256
    vmem, hbm = spec(pltpu.VMEM), spec(pltpu.HBM)
    bounds = pltpu.SMEM(old_bounds.shape, jnp.int32)
    starts = pltpu.SMEM(seg_start.shape, jnp.int32)
    rim = pltpu.VMEM((4, BLOCK, LANES), f32)
    dma = pltpu.SemaphoreType.DMA
    placed, sums = pl.pallas_call(
        functools.partial(step_kernel, axis, n),
        name="step",
        out_shape=(
            jax.ShapeDtypeStruct((4, rows, LANES), f32),
            jax.ShapeDtypeStruct((1, LANES), f32),
        ),
        in_specs=[hbm] * 7,
        out_specs=(vmem,) * 2,
        scratch_shapes=[
            pltpu.VMEM((4, rows + 2 * PAD, LANES), f32),
            pltpu.VMEM((rows, LANES), f32),
            pltpu.VMEM((rows, LANES), f32),
            pltpu.VMEM((rows, LANES), grads.dtype),
            pltpu.VMEM((padded, 4 * LANES), jnp.bfloat16),
            pltpu.VMEM((3 * segs, padded), jnp.bfloat16),
            pltpu.VMEM((segs, LANES), jnp.int32),
            pltpu.VMEM((segs, LANES), jnp.int32),
            pltpu.VMEM((1, LANES), f32),
            rim,
            rim,
            rim,
            rim,
            pltpu.VMEM((4, EDGE, LANES), f32),
            pltpu.VMEM((4, EDGE, LANES), f32),
            pltpu.VMEM((n, 1, LANES), f32),
            bounds,
            bounds,
            starts,
            dma((4, 4)),
            dma((3,)),
            dma((n,)),
            dma((n,)),
            dma((2,)),
            dma((2,)),
        ],
        compiler_params=pltpu.CompilerParams(
            collective_id=0, has_side_effects=True, vmem_limit_bytes=VMEM_LIMIT
        ),
    )(old_bounds, new_bounds, seg_start, *flat)
    whole = jax.ShapeDtypeStruct((rows, LANES), f32)
    outs = pl.pallas_call(
        functools.partial(apply_kernel, axis),
        name="apply",
        out_shape=(whole,) * 3,
        in_specs=[hbm, hbm, vmem, vmem],
        out_specs=(hbm,) * 3,
        scratch_shapes=[pltpu.VMEM((rows, LANES), f32), bounds, starts, dma((3,)), dma((2,))],
        compiler_params=pltpu.CompilerParams(vmem_limit_bytes=VMEM_LIMIT),
    )(new_bounds, seg_start, placed, sums)
    return tuple(x.reshape(cap) for x in outs)


def solution(mesh):
    (axis,) = mesh.axis_names
    n = mesh.shape[axis]
    placed = (P(axis), P(axis), P(axis), P(axis), P(), P(), P())
    return jax.shard_map(
        functools.partial(shards, axis, n),
        mesh=mesh,
        in_specs=placed,
        out_specs=(P(axis), P(axis), P(axis)),
        check_vma=False,
    )
```

```python
import functools

import jax
import jax.numpy as jnp
from jax import lax
from jax.experimental import pallas as pl
from jax.experimental.pallas import tpu as pltpu
from jax.sharding import PartitionSpec as P

MARGIN = 4096
LANES = 128
BLOCK = MARGIN // LANES
HALF = 64
HALF_BITS = 6
LANE_BITS = 7
PAD = BLOCK + 8
EDGE = 2 * PAD + BLOCK


BETA_ONE = 0.9
BETA_TWO = 0.999
CORR_ONE = 1.0 - 0.9**10
CORR_TWO = 1.0 - 0.999**10
DECAY = 0.01
LEARN = 0.1
EPSILON = 1e-06

MESH = pl.DeviceIdType.MESH
VMEM_LIMIT = 16 * 1024 * 1024


def lane_ids(rows=BLOCK):
    return lax.broadcasted_iota(jnp.int32, (rows, LANES), 1)


def flat_ids():
    return lax.broadcasted_iota(jnp.int32, (BLOCK, LANES), 0) * LANES + lane_ids()


def moved(first, second, lanes):
    picked = jnp.where(lane_ids() >= lanes, first, second)
    return pltpu.roll(picked, (LANES - lanes) & (LANES - 1), 1)


def fetched(tables, refs, sems):
    copies = [pltpu.make_async_copy(t, r, sems.at[i]) for i, (t, r) in enumerate(zip(tables, refs))]
    for copy in copies:
        copy.start()
    return copies


def step_kernel(
    axis, n, old_hbm, new_hbm, seg_hbm, w_hbm, m_hbm, v_hbm, g_hbm, placed, sums, chosen,
    state, m_buf, v_buf, g_buf, squares, member, begins, ends, part, tail, head, left_rim, right_rim,
    before, after, slots, old_ref, new_ref, seg_ref, sems, table_sems, send, receive, rim_send, rim_receive,
):
    rows = m_buf.shape[0]
    blocks = rows // BLOCK
    segs = seg_ref.shape[0]
    me = lax.axis_index(axis)
    right = lax.rem(me + 1, n)
    left = lax.rem(me + n - 1, n)
    tables = fetched((old_hbm, new_hbm, seg_hbm), (old_ref, new_ref, seg_ref), table_sems)
    step_blocks = -(-blocks // sems.shape[1])
    chunks = [(b, min(b + step_blocks, blocks)) for b in range(0, blocks, step_blocks)]
    copies = []
    for c, (b0, b1) in enumerate(chunks):
        window = pl.ds(b0 * BLOCK, (b1 - b0) * BLOCK)
        inside = state.at[0, pl.ds(PAD + b0 * BLOCK, (b1 - b0) * BLOCK)]
        group = [
            pltpu.make_async_copy(w_hbm.at[window], inside, sems.at[0, c]),
            pltpu.make_async_copy(m_hbm.at[window], m_buf.at[window], sems.at[1, c]),
            pltpu.make_async_copy(v_hbm.at[window], v_buf.at[window], sems.at[2, c]),
            pltpu.make_async_copy(g_hbm.at[window], g_buf.at[window], sems.at[3, c]),
        ]
        for copy in group:
            copy.start()
        copies.append(group)

    barrier = pltpu.get_barrier_semaphore()

    def greet(k, carry):
        pl.semaphore_signal(barrier, inc=1, device_id=(lax.rem(me + k, n),), device_id_type=MESH)
        return carry

    lax.fori_loop(1, n, greet, 0)

    for copy in tables:
        copy.wait()
    low = old_ref[me]
    count = old_ref[me + 1] - low
    new_low = new_ref[me]
    new_count = new_ref[me + 1] - new_low
    shift = new_low - low
    phase = (-low) & (HALF - 1)

    def bound_all(origin, offset):
        def bound(s, carry):
            value = (seg_ref[s] - origin - offset) >> HALF_BITS
            begins[pl.ds(s, 1), :] = jnp.full((1, LANES), value, jnp.int32)
            following = (seg_ref[jnp.minimum(s + 1, segs - 1)] - origin - offset) >> HALF_BITS
            following = jnp.where(s + 1 < segs, following, 4 * rows)
            ends[pl.ds(s, 1), :] = jnp.full((1, LANES), following, jnp.int32)
            return carry

        lax.fori_loop(0, segs, bound, 0, unroll=8)

    bound_all(low, phase)
    padded = member.shape[1]
    spot = lane_ids(segs)
    first_half = begins[...]
    past_half = ends[...]
    for group in range(3):
        for tile in range(padded // LANES):
            half = 2 * (spot + tile * LANES) - 1 + group
            mask = (half >= first_half) & (half < past_half)
            member[group * segs : (group + 1) * segs, tile * LANES : (tile + 1) * LANES] = jnp.where(
                mask, 1.0, 0.0
            ).astype(jnp.bfloat16)
    squares[rows:padded, :] = jnp.zeros((padded - rows, 4 * LANES), jnp.bfloat16)

    flat = flat_ids()

    def advance(b, carry):
        here = pl.multiple_of(b * BLOCK, BLOCK)
        there = pl.multiple_of(b * BLOCK + PAD, 8)
        gradient = g_buf[pl.ds(here, BLOCK), :].astype(jnp.float32)
        weight = state[0, pl.ds(there, BLOCK), :]
        moment = BETA_ONE * m_buf[pl.ds(here, BLOCK), :] + (1.0 - BETA_ONE) * gradient
        second = BETA_TWO * v_buf[pl.ds(here, BLOCK), :] + (1.0 - BETA_TWO) * gradient * gradient
        scaled = moment * (1.0 / CORR_ONE)
        update = scaled / (jnp.sqrt(second * (1.0 / CORR_TWO)) + EPSILON) + DECAY * weight
        state[1, pl.ds(there, BLOCK), :] = update
        state[2, pl.ds(there, BLOCK), :] = moment
        state[3, pl.ds(there, BLOCK), :] = second
        live = flat + b * MARGIN < count
        for i, value in enumerate((weight, update)):
            square = jnp.where(live, value * value, 0.0)
            coarse = square.astype(jnp.bfloat16)
            fine = (square - coarse.astype(jnp.float32)).astype(jnp.bfloat16)
            squares[pl.ds(here, BLOCK), i * LANES : (i + 1) * LANES] = coarse
            squares[pl.ds(here, BLOCK), (i + 2) * LANES : (i + 3) * LANES] = fine
        return carry

    for (b0, b1), group in zip(chunks, copies):
        for copy in group:
            copy.wait()
        lax.fori_loop(b0, b1, advance, 0, unroll=2)

    start = count - MARGIN
    start_row = start >> LANE_BITS
    start_lane = start & (LANES - 1)
    for a in range(4):
        head[a] = state[a, PAD : PAD + BLOCK, :]
        tail[a] = moved(
            state[a, pl.ds(PAD + start_row, BLOCK), :],
            state[a, pl.ds(PAD + start_row + 1, BLOCK), :],
            start_lane,
        )

    product = jnp.dot(member[...], squares[...], preferred_element_type=jnp.float32)
    product = product[:, : 2 * LANES] + product[:, 2 * LANES :]
    line = lax.broadcasted_iota(jnp.int32, (segs, LANES), 0)
    row = jnp.zeros((segs, LANES), jnp.float32)
    for i in range(2):
        columns = slice(i * LANES, (i + 1) * LANES)
        mixed = jnp.where(
            spot < phase,
            product[0:segs, columns],
            jnp.where(
                spot < phase + HALF, product[segs : 2 * segs, columns], product[2 * segs : 3 * segs, columns]
            ),
        )
        row = jnp.where(spot == line + i * segs, jnp.sum(mixed, axis=1, keepdims=True), row)
    part[...] = jnp.sum(row, axis=0, keepdims=True)
    pl.semaphore_wait(barrier, n - 1)

    def tell(k):
        return pltpu.make_async_remote_copy(
            src_ref=part,
            dst_ref=slots.at[me],
            send_sem=send,
            recv_sem=receive,
            device_id=(lax.rem(me + k, n),),
            device_id_type=MESH,
        )

    onward = pltpu.make_async_remote_copy(
        src_ref=tail,
        dst_ref=left_rim,
        send_sem=rim_send.at[0],
        recv_sem=rim_receive.at[0],
        device_id=(right,),
        device_id_type=MESH,
    )
    back = pltpu.make_async_remote_copy(
        src_ref=head,
        dst_ref=right_rim,
        send_sem=rim_send.at[1],
        recv_sem=rim_receive.at[1],
        device_id=(left,),
        device_id_type=MESH,
    )

    for k in range(1, n):
        tell(k).start()
    pltpu.make_async_copy(part, slots.at[me], receive).start()
    onward.start()
    back.start()

    top = shift >> LANE_BITS
    lanes = shift & (LANES - 1)

    def own(a, b):
        there = b * BLOCK + PAD + top
        return moved(state[a, pl.ds(there, BLOCK), :], state[a, pl.ds(there + 1, BLOCK), :], lanes)

    def inner(b, carry):
        here = pl.multiple_of(b * BLOCK, BLOCK)
        for a in range(4):
            placed[a, pl.ds(here, BLOCK), :] = own(a, b)
        return carry

    lax.fori_loop(1, blocks - 3, inner, 0, unroll=3)
    for a in range(4):
        before[a, BLOCK:EDGE, :] = state[a, PAD : PAD + EDGE - BLOCK, :]
    onward.wait()
    back.wait()
    for a in range(4):
        before[a, 0:BLOCK, :] = left_rim[a]
        after[a, PAD : PAD + BLOCK, :] = right_rim[a]
    for a in range(4):
        placed[a, 0:BLOCK, :] = moved(
            before[a, pl.ds(BLOCK + top, BLOCK), :], before[a, pl.ds(BLOCK + top + 1, BLOCK), :], lanes
        )

    for b in range(blocks - 3, blocks):
        offset = b * MARGIN + shift - count
        near = jnp.clip(offset >> LANE_BITS, -PAD, PAD - 7) + PAD
        side = offset & (LANES - 1)
        index = flat + b * MARGIN
        beyond = index + shift >= count
        live = index < new_count
        for a in range(4):
            rim = moved(after[a, pl.ds(near, BLOCK), :], after[a, pl.ds(near + 1, BLOCK), :], side)
            value = jnp.where(beyond, rim, own(a, b))
            placed[a, b * BLOCK : (b + 1) * BLOCK, :] = jnp.where(live, value, 0.0)

    new_phase = (-new_low) & (HALF - 1)
    bound_all(new_low, new_phase)
    on_lane = (spot & (segs - 1)) == line
    lows = jnp.sum(jnp.where(on_lane, begins[...], 0), axis=0, keepdims=True)
    highs = jnp.sum(jnp.where(on_lane, ends[...], 0), axis=0, keepdims=True)
    block_row = lax.broadcasted_iota(jnp.int32, (BLOCK, LANES), 0)
    lane_group = lane_ids() >> HALF_BITS

    def choose(b, carry):
        here = pl.multiple_of(b * BLOCK, BLOCK)
        for tile in range(2):
            half = 2 * (block_row + b * BLOCK) - 1 + 2 * tile + lane_group
            mask = (half >= lows) & (half < highs)
            chosen[pl.ds(here, BLOCK), tile * LANES : (tile + 1) * LANES] = jnp.where(mask, 1.0, 0.0).astype(
                jnp.bfloat16
            )
        return carry

    lax.fori_loop(0, blocks, choose, 0, unroll=2)
    sums[1:2, :] = jnp.full((1, LANES), new_phase, jnp.int32).astype(jnp.float32)

    pltpu.make_async_copy(slots, slots, receive).wait()
    sums[0:1, :] = jnp.sum(slots[...], axis=0)
    others = slots.at[pl.ds(0, n - 1)]
    pltpu.make_async_copy(others, others, send).wait()


def apply_kernel(segs, placed, sums, chosen, w_out, m_out, v_out, w_buf, sems):
    m_copy = pltpu.make_async_copy(placed.at[2], m_out, sems.at[0])
    v_copy = pltpu.make_async_copy(placed.at[3], v_out, sems.at[1])
    m_copy.start()
    v_copy.start()
    rows = w_buf.shape[0]
    total = sums[0:1, :]
    phase = sums[1:2, :]
    other = pltpu.roll(total, LANES - segs, 1)
    rate = LEARN * (jnp.sqrt(total) / (jnp.sqrt(other) + EPSILON))
    spot = lane_ids(segs)
    line = lax.broadcasted_iota(jnp.int32, (segs, LANES), 0)
    column = jnp.sum(jnp.where(spot == line, rate, 0.0), axis=1, keepdims=True)
    place = spot.astype(jnp.float32)
    early = place < phase
    late = place >= phase + HALF
    nothing = jnp.zeros((segs, LANES), jnp.float32)
    rates = jnp.concatenate(
        [
            jnp.where(early, column, 0.0),
            jnp.where(early | late, 0.0, column),
            jnp.where(late, column, 0.0),
            nothing,
        ],
        axis=0,
    )
    coarse = rates.astype(jnp.bfloat16)
    fine = (rates - coarse.astype(jnp.float32)).astype(jnp.bfloat16)
    table = jnp.concatenate([coarse, fine], axis=1)
    step = 256
    copies = []
    for c, r0 in enumerate(range(0, rows, step)):
        size = min(step, rows - r0)
        product = jnp.dot(chosen[r0 : r0 + size, :], table, preferred_element_type=jnp.float32)
        factor = product[:, :LANES] + product[:, LANES:]
        w_buf[r0 : r0 + size, :] = placed[0, r0 : r0 + size, :] - factor * placed[1, r0 : r0 + size, :]
        window = pl.ds(r0, size)
        copy = pltpu.make_async_copy(w_buf.at[window], w_out.at[window], sems.at[2 + c])
        copy.start()
        copies.append(copy)
    for copy in (m_copy, v_copy, *copies):
        copy.wait()


def spec(space):
    return pl.BlockSpec(memory_space=space)


def shards(axis, n, params, first_moment, second_moment, grads, old_bounds, new_bounds, seg_start):
    cap = params.shape[0]
    rows = cap // LANES
    f32 = jnp.float32
    flat = [x.reshape(rows, LANES) for x in (params, first_moment, second_moment, grads)]
    old_bounds, new_bounds, seg_start, *flat = (
        pltpu.with_memory_space_constraint(x, pltpu.HBM) for x in (old_bounds, new_bounds, seg_start, *flat)
    )
    segs = seg_start.shape[0]
    padded = -(-rows // 256) * 256
    vmem, hbm = spec(pltpu.VMEM), spec(pltpu.HBM)
    bounds = pltpu.SMEM(old_bounds.shape, jnp.int32)
    starts = pltpu.SMEM(seg_start.shape, jnp.int32)
    rim = pltpu.VMEM((4, BLOCK, LANES), f32)
    dma = pltpu.SemaphoreType.DMA
    placed, sums, chosen = pl.pallas_call(
        functools.partial(step_kernel, axis, n),
        name="step",
        out_shape=(
            jax.ShapeDtypeStruct((4, rows, LANES), f32),
            jax.ShapeDtypeStruct((2, LANES), f32),
            jax.ShapeDtypeStruct((rows, 2 * LANES), jnp.bfloat16),
        ),
        in_specs=[hbm] * 7,
        out_specs=(vmem,) * 3,
        scratch_shapes=[
            pltpu.VMEM((4, rows + 2 * PAD, LANES), f32),
            pltpu.VMEM((rows, LANES), f32),
            pltpu.VMEM((rows, LANES), f32),
            pltpu.VMEM((rows, LANES), grads.dtype),
            pltpu.VMEM((padded, 4 * LANES), jnp.bfloat16),
            pltpu.VMEM((3 * segs, padded), jnp.bfloat16),
            pltpu.VMEM((segs, LANES), jnp.int32),
            pltpu.VMEM((segs, LANES), jnp.int32),
            pltpu.VMEM((1, LANES), f32),
            rim,
            rim,
            rim,
            rim,
            pltpu.VMEM((4, EDGE, LANES), f32),
            pltpu.VMEM((4, EDGE, LANES), f32),
            pltpu.VMEM((n, 1, LANES), f32),
            bounds,
            bounds,
            starts,
            dma((4, 2)),
            dma((3,)),
            dma,
            dma,
            dma((2,)),
            dma((2,)),
        ],
        compiler_params=pltpu.CompilerParams(
            collective_id=0, has_side_effects=True, vmem_limit_bytes=VMEM_LIMIT
        ),
    )(old_bounds, new_bounds, seg_start, *flat)
    whole = jax.ShapeDtypeStruct((rows, LANES), f32)
    outs = pl.pallas_call(
        functools.partial(apply_kernel, segs),
        name="apply",
        out_shape=(whole,) * 3,
        in_specs=[vmem] * 3,
        out_specs=(hbm,) * 3,
        scratch_shapes=[pltpu.VMEM((rows, LANES), f32), dma((2 + -(-rows // 256),))],
        compiler_params=pltpu.CompilerParams(vmem_limit_bytes=VMEM_LIMIT),
    )(placed, sums, chosen)
    return tuple(x.reshape(cap) for x in outs)


def solution(mesh):
    (axis,) = mesh.axis_names
    n = mesh.shape[axis]
    placed = (P(axis), P(axis), P(axis), P(axis), P(), P(), P())
    return jax.shard_map(
        functools.partial(shards, axis, n),
        mesh=mesh,
        in_specs=placed,
        out_specs=(P(axis), P(axis), P(axis)),
        check_vma=False,
    )
```
